32 devices in a mesh: lat: 2 (over core), lon: 2 (over y), lev: 2 (over x), unit: 4 (over z).
Axes of the slice: x: 2, y: 2, z: 4, core: 2. Of those that a mesh axis runs over, the one named last changes fastest.
Arguments:
- tracer: float32 [32, 256, 32, 128], P(('unit', 'lat'), 'lon', 'lev'), parts along dimension 0, may hold values from 0.5 to 2
- diffusivity: float32 [32, 256, 32, 128], P(('unit', 'lat'), 'lon', 'lev'), parts along dimension 0, may hold values from 0.03 to 0.15
- source: float32 [32, 256, 32, 128], P(('unit', 'lat'), 'lon', 'lev'), parts along dimension 0, may hold values from -0.2 to 0.2
Outputs:
- standardized: float32 [32, 256, 32, 128], P(('unit', 'lat'), 'lon', 'lev'), parts along dimension 0
- tracer_end: float32 [32, 256, 32, 128], P(('unit', 'lat'), 'lon', 'lev'), parts along dimension 0
The draws below stay inside these ranges and needn't reach their ends.
There are 4 independent parts, one for each index of `unit`. The reference program is written for one: setup_inputs(seed, part) draws one part's arguments, and reference() takes and returns one part's arrays. A program takes and returns all parts, laid end to end along the dimension named above; each array names one. Nothing has to cross between parts.
All inputs are finite; a program needn't handle non-finite values.
Results may differ from the reference program's by a relative error of at most 0.00002.
Values sent between devices are 32-bit elements; how exact they have to be, the bound alone decides.
No kernel may reach another device: no remote copies, remote signals or barrier semaphores. Data moves between devices by JAX's collectives and lax.ppermute only.
A program may use at most 128 MiB of HBM per device.

```python
import jax
import jax.numpy as jnp
from jax import lax

GRID_J = 8
GRID_I = 256
GRID_K = 32
LEVELS = 128
STEPS = 4


def steps_of(rng, extent, split, smallest, largest):
    gain = 1.0
    for dim, parts in split:
        steps = jax.random.uniform(jax.random.fold_in(jax.random.fold_in(rng, 6), dim), (parts,), jnp.float32, smallest / len(split), largest / len(split))
        gain = gain * jnp.repeat(jnp.exp(steps), extent[dim] // parts).reshape((-1,) + (1,) * (len(extent) - 1 - dim))
    return gain


def setup_inputs(seed: int = 0, part: int = 0) -> dict:
    streams_of = jax.random.split(jax.random.key(seed), 4)
    part_keys = jax.random.split(jax.random.fold_in(streams_of[3], part), 4)
    return {
        "tracer": jnp.clip(0.5 + 1.5 * jax.random.uniform(part_keys[0], (GRID_J, GRID_I, GRID_K, LEVELS), jnp.float32) ** steps_of(part_keys[0], (GRID_J, GRID_I, GRID_K, LEVELS), ((0, 2), (1, 2), (2, 2)), -0.2, 0.2), 0.5, 2.0),
        "diffusivity": jnp.clip(0.03 + 0.120000007 * jax.random.uniform(part_keys[1], (GRID_J, GRID_I, GRID_K, LEVELS), jnp.float32) ** steps_of(part_keys[1], (GRID_J, GRID_I, GRID_K, LEVELS), ((0, 2), (1, 2), (2, 2)), -0.2, 0.2), 0.03, 0.15),
        "source": jnp.clip(jax.random.uniform(part_keys[2], (GRID_J, GRID_I, GRID_K, LEVELS), jnp.float32, -0.2, 0.2) * steps_of(part_keys[2], (GRID_J, GRID_I, GRID_K, LEVELS), ((0, 2), (1, 2), (2, 2)), -0.4, 0.0), -0.2, 0.2),
    }


def strip_edges(values, dims):
    for dim in dims:
        values = lax.slice_in_dim(values, 1, values.shape[dim] - 1, axis=dim)
    return values

def neighbour(values, dim, start, dims):
    others = [other for other in dims if other != dim]
    values = strip_edges(values, others)
    return lax.slice_in_dim(values, start, start + values.shape[dim] - 2, axis=dim)

def one_step(padded, diffusivity, source):
    middle = strip_edges(padded, (0, 1, 2))
    lower = [neighbour(padded, dim, 0, (0, 1, 2)) for dim in (0, 1, 2)]
    upper = [neighbour(padded, dim, 2, (0, 1, 2)) for dim in (0, 1, 2)]
    spread = lower[0] + upper[0] + lower[1] + upper[1] + lower[2] + upper[2] - 6.0 * middle
    return middle + diffusivity * spread + source

def reference(tracer, diffusivity, source):
    for step in range(STEPS):
        tracer = one_step(jnp.pad(tracer, ((1, 1), (1, 1), (1, 1), (0, 0)), mode='wrap'), diffusivity, source)
    line_mean = lax.optimization_barrier(jnp.mean(tracer, axis=2, keepdims=True))
    centred = tracer - line_mean
    line_variance = lax.optimization_barrier(jnp.mean(centred * centred, axis=2, keepdims=True))
    standardized = centred * lax.rsqrt(line_variance + 0.0001)
    return (standardized, tracer)
```

```python
import functools

import jax
import jax.numpy as jnp
from jax import lax
from jax.experimental import pallas as pl
from jax.experimental.pallas import tpu as pltpu
from jax.sharding import PartitionSpec as P

STEPS = 4
EPSILON = 1e-4
SUB = 8
ROWS = 4
WHOLE = pl.BlockSpec(memory_space=pltpu.VMEM)
ANY = pl.BlockSpec(memory_space=pl.ANY)
F32 = jnp.float32


def in_vmem(x):
    return pltpu.with_memory_space_constraint(x, pltpu.VMEM)


def exchange(pair, axis):
    count = lax.axis_size(axis)
    forward = [(i, (i + 1) % count) for i in range(count)]
    backward = [(target, source) for source, target in forward]
    if count == 2:
        return lax.ppermute(pair, axis, forward)
    return jnp.stack(
        [lax.ppermute(pair[0], axis, forward), lax.ppermute(pair[1], axis, backward)]
    )


def others(values, axis):
    count = lax.axis_size(axis)
    return [
        lax.ppermute(values, axis, [(i, (i + shift) % count) for i in range(count)])
        for shift in range(1, count)
    ]


def plan(extent):
    quarter = extent // 4
    return (
        ((0, quarter), (extent - quarter, quarter)),
        ((quarter, extent - 2 * quarter),),
    )


def place(chunks, row):
    for number, chunk in enumerate(chunks):
        base = 0
        for first, count in chunk:
            if first <= row < first + count:
                return number, base + row - first
            base += count
    return None


def step_kernel(shape, chunks, number, start, last, *refs):
    rows_j, extent, depth, lanes = shape
    tiles = depth // SUB
    chunk = chunks[number]
    ends = number == 0
    refs = list(refs)
    fields = [refs.pop(0) for _ in range(1 if start else len(chunks))]
    diffusivity, source, lev, lat = [refs.pop(0) for _ in range(4)]
    lon = refs.pop(0) if ends else None
    result = refs.pop(0)
    if last:
        (stats,) = refs
    else:
        faces, planes = refs[:2]
        edge = refs[2] if ends else None

    sub = lax.broadcasted_iota(jnp.int32, (SUB, lanes), 0)
    first_sub, last_sub = sub == 0, sub == SUB - 1

    def load(ref, *index):
        return [ref[(*index, pl.ds(SUB * t, SUB), slice(None))] for t in range(tiles)]

    def field_row(row, offset=0):
        if row < 0 or row >= extent:
            return [load(lon, 0 if row < 0 else 1, j) for j in range(rows_j)]
        which, local = (0, row) if start else place(chunks, row)
        return [load(fields[which], j, local) for j in range(rows_j)]

    base = 0
    for first, count in chunk:
        own, own_base = (fields[0], first) if start else (fields[number], base)

        def one_row(before, now, after, r, base=base, first=first):
            at = base + r
            below = load(lat, 0, at)
            above = load(lat, 1, at)
            for j in range(rows_j):
                low = lev.at[0, j][pl.ds(at, SUB, stride=0), :]
                high = lev.at[1, j][pl.ds(at, SUB, stride=0), :]
                up = [pltpu.roll(now[j][t], 1, 0) for t in range(tiles)]
                down = [pltpu.roll(now[j][t], SUB - 1, 0) for t in range(tiles)]
                factor = load(diffusivity, j, first + r)
                added = load(source, j, first + r)
                made = []
                for t in range(tiles):
                    spread = (below if j == 0 else now[j - 1])[t]
                    spread = spread + (above if j == rows_j - 1 else now[j + 1])[t]
                    spread = spread + (before[j][t] + after[j][t])
                    spread = spread + jnp.where(first_sub, low if t == 0 else up[t - 1], up[t])
                    spread = spread + jnp.where(
                        last_sub, high if t == tiles - 1 else down[t + 1], down[t]
                    )
                    spread = spread - 6.0 * now[j][t]
                    value = now[j][t] + factor[t] * spread + added[t]
                    made.append(value)
                    result[j, at, pl.ds(SUB * t, SUB), :] = value
                if last:
                    total = functools.reduce(jnp.add, made)
                    mean = jnp.sum(total, axis=0, keepdims=True) * (1.0 / depth)
                    square = functools.reduce(jnp.add, [(v - mean) * (v - mean) for v in made])
                    stats[0, j, pl.ds(at, 1), :] = mean
                    stats[1, j, pl.ds(at, 1), :] = jnp.sum(square, axis=0, keepdims=True)
                    continue
                faces[0, j, pl.ds(at, 1), :] = made[-1][SUB - 1 :]
                faces[1, j, pl.ds(at, 1), :] = made[0][:1]
                for side, plane in ((0, rows_j - 1), (1, 0)):
                    if j == plane:
                        for t in range(tiles):
                            planes[side, at, pl.ds(SUB * t, SUB), :] = made[t]

        def block(r0, before, now, final, own=own, own_base=own_base, one_row=one_row):
            for s in range(ROWS):
                if final is not None and s == ROWS - 1:
                    after = final
                else:
                    after = [load(own, j, own_base + r0 + s + 1) for j in range(rows_j)]
                one_row(before, now, after, r0 + s)
                before, now = now, after
            return before, now

        carry = (field_row(first - 1), field_row(first))
        carry = lax.fori_loop(
            0,
            count // ROWS - 1,
            lambda b, c, block=block: block(b * ROWS, c[0], c[1], None),
            carry,
        )
        block(count - ROWS, carry[0], carry[1], field_row(first + count))
        if ends and not last:
            for side, row in ((0, extent - 1), (1, 0)):
                if first <= row < first + count:
                    at = base + row - first
                    for j in range(rows_j):
                        edge[side, j] = result[j, at]
        base += count


def size_of(chunk):
    return sum(count for _, count in chunk)


def take_step(chunks, number, fields, diffusivity, source, lev, lat, lon, start, last):
    shape = diffusivity.shape
    rows_j, extent, depth, lanes = shape
    rows = size_of(chunks[number])
    outs = [pltpu.VMEM((rows_j, rows, depth, lanes), F32)]
    if last:
        outs.append(jax.ShapeDtypeStruct((2, rows_j, rows, lanes), F32))
    else:
        outs.append(jax.ShapeDtypeStruct((2, rows_j, rows, lanes), F32))
        outs.append(jax.ShapeDtypeStruct((2, rows, depth, lanes), F32))
        if number == 0:
            outs.append(jax.ShapeDtypeStruct((2, rows_j, depth, lanes), F32))
    arrays = [*fields, diffusivity, source, lev, lat]
    if number == 0:
        arrays.append(lon)
    cells = rows_j * rows * depth * lanes
    return pl.pallas_call(
        functools.partial(step_kernel, shape, chunks, number, start, last),
        out_shape=outs,
        in_specs=[WHOLE] * len(arrays),
        out_specs=[WHOLE] * len(outs),
        compiler_params=pltpu.CompilerParams(vmem_limit_bytes=16 * 2**20),
        cost_estimate=pl.CostEstimate(flops=12 * cells, bytes_accessed=16 * cells, transcendentals=0),
        name=f"step_{number}{'_last' if last else ''}",
    )(*[in_vmem(x) for x in arrays])


def store_kernel(chunk, field, *refs):
    out, sems = refs[-2:]
    base, copies = 0, []
    for index, (first, count) in enumerate(chunk):
        copies.append(
            pltpu.make_async_copy(
                field.at[:, pl.ds(base, count)], out.at[:, pl.ds(first, count)], sems.at[index]
            )
        )
        base += count
    for copy in copies:
        copy.start()
    for copy in copies:
        copy.wait()


def store(chunk, field, shape, into):
    arrays = [in_vmem(field)] + ([into] if into is not None else [])
    return pl.pallas_call(
        functools.partial(store_kernel, chunk),
        out_shape=jax.ShapeDtypeStruct(shape, F32),
        in_specs=[WHOLE] + [ANY] * (len(arrays) - 1),
        out_specs=pl.BlockSpec(memory_space=pltpu.HBM),
        scratch_shapes=[pltpu.SemaphoreType.DMA((len(chunk),))],
        input_output_aliases={1: 0} if into is not None else {},
        compiler_params=pltpu.CompilerParams(vmem_limit_bytes=2**20),
        cost_estimate=pl.CostEstimate(flops=10**6, bytes_accessed=8 * field.size, transcendentals=0),
        name="store",
    )(*arrays)


def scale_kernel(parts, rows, field, *refs):
    stats = refs[:parts]
    out, means, scales = refs[-3:]
    rows_j, _, depth, lanes = field.shape
    row0 = pl.multiple_of(pl.program_id(0) * rows, rows)
    for j in range(rows_j):
        local = [s[0, j, pl.ds(row0, rows), :] for s in stats]
        mean = functools.reduce(jnp.add, local) * (1.0 / parts)
        square = functools.reduce(jnp.add, [s[1, j, pl.ds(row0, rows), :] for s in stats])
        between = functools.reduce(jnp.add, [(m - mean) * (m - mean) for m in local])
        variance = (square + depth * between) * (1.0 / (parts * depth))
        means[j] = mean
        scales[j] = lax.rsqrt(variance + EPSILON)
    for j in range(rows_j):
        for r in range(rows):
            mean = means.at[j][pl.ds(r, SUB, stride=0), :]
            scale = scales.at[j][pl.ds(r, SUB, stride=0), :]
            for t in range(depth // SUB):
                value = field[j, row0 + r, pl.ds(SUB * t, SUB), :]
                out[j, r, pl.ds(SUB * t, SUB), :] = (value - mean) * scale


def scale(chunk, field, stats, shape, into):
    rows_j, extent, depth, lanes = shape
    rows = 16
    starts = []
    for first, count in chunk:
        starts += [(first + n) // rows for n in range(0, count, rows)]

    def block(g):
        index = starts[-1]
        for n in range(len(starts) - 2, -1, -1):
            index = jnp.where(g == n, starts[n], index)
        return (0, index, 0, 0)

    arrays = [in_vmem(x) for x in (field, *stats)] + ([into] if into is not None else [])
    return pl.pallas_call(
        functools.partial(scale_kernel, len(stats), rows),
        grid=(len(starts),),
        out_shape=jax.ShapeDtypeStruct(shape, F32),
        in_specs=[WHOLE] * (1 + len(stats)) + [ANY] * (len(arrays) - 1 - len(stats)),
        out_specs=pl.BlockSpec((rows_j, rows, depth, lanes), block),
        scratch_shapes=[pltpu.VMEM((rows_j, rows, lanes), F32)] * 2,
        input_output_aliases={len(arrays) - 1: 0} if into is not None else {},
        compiler_params=pltpu.CompilerParams(vmem_limit_bytes=8 * 2**20),
        cost_estimate=pl.CostEstimate(flops=10**7, bytes_accessed=8 * field.size, transcendentals=0),
        name="scale",
    )(*arrays)


def on_device(tracer, diffusivity, source):
    shape = tracer.shape
    rows_j, extent, depth, lanes = shape
    chunks = plan(extent)

    def rows_of(x, dim, chunk):
        return jnp.concatenate(
            [lax.slice_in_dim(x, first, first + count, axis=dim) for first, count in chunk], axis=dim
        )

    fields = [tracer]
    lev, lat = [], []
    for chunk in chunks:
        part = rows_of(tracer, 1, chunk)
        lev.append(exchange(jnp.stack([part[:, :, depth - 1], part[:, :, 0]]), "lev"))
        lat.append(exchange(jnp.stack([part[rows_j - 1], part[0]]), "lat"))
    lon = exchange(jnp.stack([tracer[:, extent - 1], tracer[:, 0]]), "lon")
    for step in range(STEPS):
        last = step == STEPS - 1
        made, next_lev, next_lat, next_lon = [], [], [], None
        for number in range(len(chunks)):
            outs = take_step(
                chunks, number, fields, diffusivity, source,
                lev[number], lat[number], lon, step == 0, last,
            )
            made.append(outs[0])
            if last:
                next_lev.append(outs[1])
            else:
                next_lev.append(exchange(outs[1], "lev"))
                next_lat.append(exchange(outs[2], "lat"))
                if number == 0:
                    next_lon = exchange(outs[3], "lon")
        fields, lev, lat, lon = made, next_lev, next_lat, next_lon
    stats = [[mine, *others(mine, "lev")] for mine in lev]
    end = standardized = None
    for chunk, field in zip(chunks, fields):
        end = store(chunk, field, shape, end)
    for chunk, field, stat in zip(chunks, fields, stats):
        standardized = scale(chunk, field, stat, shape, standardized)
    return (standardized, end)


def solution(mesh):
    spec = P(("unit", "lat"), "lon", "lev", None)
    return jax.shard_map(
        on_device, mesh=mesh, in_specs=(spec,) * 3, out_specs=(spec,) * 2, check_vma=False
    )
```
